16 devices in a mesh: dp: 4 (over y, z, core), tp: 4 (over x).
Axes of the slice: x: 4, y: 2, z: 1, core: 2. Of those that a mesh axis runs over, the one named last changes fastest.
The devices are a block of a 4x4x8 slice.
Arguments:
- x: bfloat16 [8192, 4096], P('dp'), parts along dimension 0
- w_gate: bfloat16 [4096, 12800], P(None, 'tp')
- w_up: bfloat16 [4096, 12800], P(None, 'tp')
- w_down: bfloat16 [12800, 4096], P('tp')
Outputs:
- output: bfloat16 [8192, 4096], P('dp'), parts along dimension 0
There are 4 independent parts. The reference program is written for one: setup_inputs(seed, part) draws one part's arguments, and reference() takes and returns one part's arrays. A program takes and returns all parts, laid end to end along the dimension named above; an argument that names none is the same for every part.
All inputs are finite; a program needn't handle non-finite values.
Results may differ from the reference program's by a relative error of at most 0.016.
Values are sent between devices in bfloat16 or wider.
A program may use at most 768 MiB of HBM per device.

```python
import jax
import jax.numpy as jnp

ROWS = 2048
D = 4096
FF = 12800


def setup_inputs(seed: int = 0, part: int = 0) -> dict:
    kx, kg, ku, kd = jax.random.split(jax.random.key(seed), 4)
    drawn = {
        "x": jax.random.normal(jax.random.fold_in(kx, part), (ROWS, D), jnp.float32),
        "w_gate": jax.random.normal(kg, (D, FF), jnp.float32) * D**-0.5,
        "w_up": jax.random.normal(ku, (D, FF), jnp.float32) * D**-0.5,
        "w_down": jax.random.normal(kd, (FF, D), jnp.float32) * FF**-0.5,
    }
    return {k: v.astype(jnp.bfloat16) for k, v in drawn.items()}


def reference(x, w_gate, w_up, w_down):
    gate = jnp.dot(x, w_gate, preferred_element_type=jnp.float32)
    up = jnp.dot(x, w_up, preferred_element_type=jnp.float32)
    hidden = (jax.nn.silu(gate) * up).astype(jnp.bfloat16)
    return jnp.dot(hidden, w_down, preferred_element_type=jnp.float32).astype(jnp.bfloat16)
```

```python
import functools

import jax
import jax.numpy as jnp
from jax import lax
from jax.experimental import pallas as pl
from jax.experimental.pallas import tpu as pltpu
from jax.sharding import PartitionSpec as P

MESH = pl.DeviceIdType.MESH
F32, BF16 = jnp.float32, jnp.bfloat16

ROWS = 256
TILE = 640
FWD_AT, OWN_AT = 1, 3
FAR, NEAR, FWD = 0, 1, 2
FIRST, SECOND, PASS = 0, 1, 2


def kernel(
    n, x_hbm, wg_hbm, wu_hbm, wd_hbm, y_hbm,
    xbuf, wbuf, dbuf, hbuf, sbuf, obuf, rbuf,
    x_sem, w_sem, d_sem, y_sem, rs_send, rs_recv, ag_send, ag_recv,
):
    rows, d_model = x_hbm.shape
    ff = wg_hbm.shape[1]
    chunks, tiles = rows // ROWS, ff // TILE
    width = d_model // n
    half = width // 2
    me = lax.axis_index("tp")
    side = (lax.rem(me + n - 1, n), lax.rem(me + 1, n))
    far = lax.rem(me + 2, n)

    def rows_of(c):
        return pl.ds(pl.multiple_of(c * ROWS, ROWS), ROWS)

    def cols_of(shard, h):
        return pl.ds(pl.multiple_of(shard * width + h * half, half), half)

    def x_copy(c):
        slot = lax.rem(c, 2)
        return pltpu.make_async_copy(x_hbm.at[rows_of(c), :], xbuf.at[slot], x_sem.at[slot])

    def w_copies(t):
        slot, j = lax.rem(t, 2), lax.rem(t, tiles)
        cols = pl.ds(pl.multiple_of(j * TILE, TILE), TILE)
        return (
            pltpu.make_async_copy(wg_hbm.at[:, cols], wbuf.at[slot, :, pl.ds(0, TILE)], w_sem.at[slot, 0]),
            pltpu.make_async_copy(wu_hbm.at[:, cols], wbuf.at[slot, :, pl.ds(TILE, TILE)], w_sem.at[slot, 1]),
        )

    pieces = (
        (far, 0), (far, 1), (side[0], 1), (side[1], 0),
        (side[0], 0), (side[1], 1), (me, 0), (me, 1),
    )

    def d_copy(q):
        slot = q % 2
        return pltpu.make_async_copy(wd_hbm.at[:, cols_of(*pieces[q])], dbuf.at[slot], d_sem.at[slot])

    def rs_copy(c, k, a):
        slot = lax.rem(c, 2)
        return pltpu.make_async_remote_copy(
            src_ref=sbuf.at[slot, 2 * k + a],
            dst_ref=rbuf.at[c, 2 * k + a],
            send_sem=rs_send.at[slot, 2 * k + a],
            recv_sem=rs_recv.at[c, 2 * k + a],
            device_id={"tp": side[a]},
            device_id_type=MESH,
        )

    def ag_copy(c, k, a):
        slot = lax.rem(c, 2)
        if k == PASS:
            where = y_hbm.at[rows_of(c), cols_of(side[1 - a], a)]
            src = where
        else:
            h = a if k == FIRST else 1 - a
            where = y_hbm.at[rows_of(c), cols_of(me, h)]
            src = obuf.at[slot, h]
        return pltpu.make_async_remote_copy(
            src_ref=src,
            dst_ref=where,
            send_sem=ag_send.at[slot, 2 * k + a],
            recv_sem=ag_recv.at[c, 2 * k + a],
            device_id={"tp": side[a]},
            device_id_type=MESH,
        )

    def y_copy(c, h):
        slot = lax.rem(c, 2)
        return pltpu.make_async_copy(
            obuf.at[slot, h], y_hbm.at[rows_of(c), cols_of(me, h)], y_sem.at[slot, h]
        )

    def term(c, q):
        if q < 7:
            d_copy(q + 1).start()
        else:
            @pl.when(c + 1 < chunks)
            def _():
                d_copy(0).start()
        d_copy(q).wait()
        return jnp.dot(hbuf[lax.rem(c, 2)], dbuf[q % 2], preferred_element_type=F32)

    def hidden(c, j):
        t = c * tiles + j

        @pl.when(t + 1 < chunks * tiles)
        def _():
            for copy in w_copies(t + 1):
                copy.start()

        @pl.when(j == 0)
        def _():
            @pl.when(c + 1 < chunks)
            def _():
                x_copy(c + 1).start()
            x_copy(c).wait()

        for copy in w_copies(t):
            copy.wait()
        both = jnp.dot(xbuf[lax.rem(c, 2)], wbuf[lax.rem(t, 2)], preferred_element_type=F32)
        gate, up = both[:, :TILE], both[:, TILE:]
        cols = pl.ds(pl.multiple_of(j * TILE, TILE), TILE)
        hbuf[lax.rem(c, 2), :, cols] = (jax.nn.silu(gate) * up).astype(BF16)

    def send_term(c, k, a, acc):
        @pl.when(c >= 2)
        def _():
            rs_copy(c - 2, k, a).wait_send()
        sbuf[lax.rem(c, 2), 2 * k + a] = acc.astype(BF16)
        rs_copy(c, k, a).start()

    def leaves(c):
        for q in range(4):
            k, a = q // 2, q % 2
            send_term(c, k, a, term(c, q))

    def forwards(c):
        for a in range(2):
            rs_copy(c, FAR, a).wait_recv()
            send_term(c, FWD, a, term(c, 4 + a) + rbuf[c, 2 * FAR + a].astype(F32))

    def own(c):
        for h in range(2):
            rs_copy(c, NEAR, 1 - h).wait_recv()
            rs_copy(c, FWD, h).wait_recv()
            acc = term(c, 6 + h) + rbuf[c, 2 * NEAR + 1 - h].astype(F32) + rbuf[c, 2 * FWD + h].astype(F32)

            @pl.when(c >= 2)
            def _():
                y_copy(c - 2, h).wait()
                ag_copy(c - 2, FIRST, h).wait_send()
                ag_copy(c - 2, SECOND, 1 - h).wait_send()
            obuf[lax.rem(c, 2), h] = acc.astype(BF16)
            y_copy(c, h).start()
            ag_copy(c, FIRST, h).start()
        for a in range(2):
            ag_copy(c, SECOND, a).start()

    def passes(c):
        for a in range(2):
            @pl.when(c >= 2)
            def _():
                ag_copy(c - 2, PASS, a).wait_send()
            ag_copy(c, FIRST, a).wait_recv()
            ag_copy(c, PASS, a).start()

    x_copy(0).start()
    for copy in w_copies(0):
        copy.start()
    d_copy(0).start()

    barrier = pltpu.get_barrier_semaphore()
    for a in range(2):
        pl.semaphore_signal(barrier, inc=1, device_id={"tp": side[a]}, device_id_type=MESH)
    pl.semaphore_wait(barrier, 2)

    @pl.loop(0, chunks + 1)
    def _(c):
        @pl.loop(0, tiles)
        def _(j):
            @pl.when(c < chunks)
            def _():
                hidden(c, j)

            @pl.when(jnp.logical_and(c >= 1, j == FWD_AT))
            def _():
                forwards(c - 1)

            @pl.when(jnp.logical_and(c >= 1, j == OWN_AT))
            def _():
                own(c - 1)

        @pl.when(c < chunks)
        def _():
            leaves(c)

        @pl.when(c >= 1)
        def _():
            passes(c - 1)

    @pl.loop(chunks - 2, chunks)
    def _(c):
        for a in range(2):
            for k in range(3):
                rs_copy(c, k, a).wait_send()
                ag_copy(c, k, a).wait_send()
            y_copy(c, a).wait()

    @pl.loop(0, chunks)
    def _(c):
        for a in range(2):
            ag_copy(c, SECOND, a).wait_recv()
            ag_copy(c, PASS, a).wait_recv()


def solution(mesh):
    n = mesh.shape["tp"]

    def step(x, w_gate, w_up, w_down):
        rows, d_model = x.shape
        ff = w_gate.shape[1]
        chunks, half = rows // ROWS, d_model // n // 2
        assert n == 4 and rows % ROWS == 0 and ff % TILE == 0
        dma = pltpu.SemaphoreType.DMA
        flops = 6 * rows * d_model * ff
        return pl.pallas_call(
            functools.partial(kernel, n),
            out_shape=jax.ShapeDtypeStruct((rows, d_model), BF16),
            in_specs=[pl.BlockSpec(memory_space=pl.ANY)] * 4,
            out_specs=pl.BlockSpec(memory_space=pl.ANY),
            scratch_shapes=[
                pltpu.VMEM((2, ROWS, d_model), BF16),
                pltpu.VMEM((2, d_model, 2 * TILE), BF16),
                pltpu.VMEM((2, ff, half), BF16),
                pltpu.VMEM((2, ROWS, ff), BF16),
                pltpu.VMEM((2, 6, ROWS, half), BF16),
                pltpu.VMEM((2, 2, ROWS, half), BF16),
                pltpu.VMEM((chunks, 6, ROWS, half), BF16),
                dma((2,)), dma((2, 2)), dma((2,)), dma((2, 2)),
                dma((2, 6)), dma((chunks, 6)), dma((2, 6)), dma((chunks, 6)),
            ],
            compiler_params=pltpu.CompilerParams(
                collective_id=0, has_side_effects=True, vmem_limit_bytes=62 * 1024 * 1024
            ),
            cost_estimate=pl.CostEstimate(
                flops=flops, bytes_accessed=chunks * 6 * d_model * ff, transcendentals=rows * ff
            ),
        )(x, w_gate, w_up, w_down)

    return jax.shard_map(
        step,
        mesh=mesh,
        in_specs=(P("dp", None), P(None, "tp"), P(None, "tp"), P("tp", None)),
        out_specs=P("dp", None),
        check_vma=False,
    )
```

```python
import functools

import jax
import jax.numpy as jnp
from jax import lax
from jax.experimental import pallas as pl
from jax.experimental.pallas import tpu as pltpu
from jax.sharding import PartitionSpec as P

MESH = pl.DeviceIdType.MESH
F32, BF16 = jnp.float32, jnp.bfloat16

ROWS = 256
TILE = 640
FWD_AT, OWN_AT = 0, 2
FAR, NEAR, FWD = 0, 1, 2
FIRST, SECOND, PASS = 0, 1, 2


def kernel(
    n, x_hbm, wg_hbm, wu_hbm, wd_hbm, y_ref,
    xbuf, wbuf, dbuf, hbuf, sbuf, nbuf,
    x_sem, w_sem, d_sem, rs_send, rs_recv, ag_send, ag_recv,
):
    rows, d_model = x_hbm.shape
    ff = wg_hbm.shape[1]
    chunks, tiles = rows // ROWS, ff // TILE
    width = d_model // n
    half = width // 2
    me = lax.axis_index("tp")
    side = (lax.rem(me + n - 1, n), lax.rem(me + 1, n))
    far = lax.rem(me + 2, n)

    def rows_of(c):
        return pl.ds(pl.multiple_of(c * ROWS, ROWS), ROWS)

    def cols_of(shard, h):
        return pl.ds(pl.multiple_of(shard * width + h * half, half), half)

    def x_copy(c):
        slot = lax.rem(c, 2)
        return pltpu.make_async_copy(x_hbm.at[rows_of(c), :], xbuf.at[slot], x_sem.at[slot])

    def w_copies(t):
        slot, j = lax.rem(t, 2), lax.rem(t, tiles)
        cols = pl.ds(pl.multiple_of(j * TILE, TILE), TILE)
        return (
            pltpu.make_async_copy(wg_hbm.at[:, cols], wbuf.at[slot, :, pl.ds(0, TILE)], w_sem.at[slot, 0]),
            pltpu.make_async_copy(wu_hbm.at[:, cols], wbuf.at[slot, :, pl.ds(TILE, TILE)], w_sem.at[slot, 1]),
        )

    pieces = (
        (far, 0), (far, 1), (side[0], 1), (side[1], 0),
        (side[0], 0), (side[1], 1), (me, 0), (me, 1),
    )

    def d_copy(q):
        slot = q % 2
        return pltpu.make_async_copy(wd_hbm.at[:, cols_of(*pieces[q])], dbuf.at[slot], d_sem.at[slot])

    def place(c, shard, h):
        return y_ref.at[rows_of(c), cols_of(shard, h)]

    def send(src, dst, send_sem, recv_sem, a):
        return pltpu.make_async_remote_copy(
            src_ref=src, dst_ref=dst, send_sem=send_sem, recv_sem=recv_sem,
            device_id={"tp": side[a]}, device_id_type=MESH,
        )

    def rs_copy(c, k, a):
        slot, i = lax.rem(c, 2), 2 * k + a
        if k == FAR:
            dst = place(c, far, a)
        elif k == NEAR:
            dst = nbuf.at[c, a]
        else:
            dst = place(c, side[a], a)
        return send(sbuf.at[slot, i], dst, rs_send.at[slot, i], rs_recv.at[c, i], a)

    def ag_copy(c, k, a):
        if k == PASS:
            where = place(c, side[1 - a], a)
        else:
            where = place(c, me, a if k == FIRST else 1 - a)
        return send(where, where, ag_send.at[lax.rem(c, 2), 2 * k + a], ag_recv.at[c, 2 * k + a], a)

    def term(c, q):
        if q < 7:
            d_copy(q + 1).start()
        else:
            @pl.when(c + 1 < chunks)
            def _():
                d_copy(0).start()
        d_copy(q).wait()
        return jnp.dot(hbuf[lax.rem(c, 2)], dbuf[q % 2], preferred_element_type=F32)

    def hidden(c, j):
        t = c * tiles + j

        @pl.when(t + 1 < chunks * tiles)
        def _():
            for copy in w_copies(t + 1):
                copy.start()

        @pl.when(j == 0)
        def _():
            @pl.when(c + 1 < chunks)
            def _():
                x_copy(c + 1).start()
            x_copy(c).wait()

        for copy in w_copies(t):
            copy.wait()
        both = jnp.dot(xbuf[lax.rem(c, 2)], wbuf[lax.rem(t, 2)], preferred_element_type=F32)
        gate, up = both[:, :TILE], both[:, TILE:]
        cols = pl.ds(pl.multiple_of(j * TILE, TILE), TILE)
        hbuf[lax.rem(c, 2), :, cols] = (jax.nn.silu(gate) * up).astype(BF16)

    def free(c, copies):
        @pl.when(c >= 2)
        def _():
            for copy, k, a in copies:
                copy(c - 2, k, a).wait_send()

    def leaves(c):
        for q in range(4):
            k, a = q // 2, q % 2
            free(c, [(rs_copy, k, a)])
            sbuf[lax.rem(c, 2), 2 * k + a] = term(c, q).astype(BF16)
            rs_copy(c, k, a).start()

    def forwards(c):
        for a in range(2):
            free(c, [(rs_copy, FWD, a)])
            rs_copy(c, FAR, a).wait_recv()
            total = term(c, 4 + a) + y_ref[rows_of(c), cols_of(side[a], a)].astype(F32)
            sbuf[lax.rem(c, 2), 2 * FWD + a] = total.astype(BF16)
            rs_copy(c, FWD, a).start()

    def own(c):
        for h in range(2):
            free(c, [(ag_copy, FIRST, h), (ag_copy, SECOND, 1 - h)])
            at = (rows_of(c), cols_of(me, h))
            rs_copy(c, NEAR, 1 - h).wait_recv()
            rs_copy(c, FWD, h).wait_recv()
            total = term(c, 6 + h) + nbuf[c, 1 - h].astype(F32) + y_ref[at].astype(F32)
            y_ref[at] = total.astype(BF16)
            ag_copy(c, FIRST, h).start()
        for a in range(2):
            ag_copy(c, SECOND, a).start()

    def passes(c):
        for a in range(2):
            free(c, [(ag_copy, PASS, a)])
            ag_copy(c, FIRST, a).wait_recv()
            ag_copy(c, PASS, a).start()

    x_copy(0).start()
    for copy in w_copies(0):
        copy.start()
    d_copy(0).start()

    barrier = pltpu.get_barrier_semaphore()
    for a in range(2):
        pl.semaphore_signal(barrier, inc=1, device_id={"tp": side[a]}, device_id_type=MESH)
    pl.semaphore_wait(barrier, 2)

    @pl.loop(0, chunks + 1)
    def _(c):
        @pl.loop(0, tiles)
        def _(j):
            @pl.when(c < chunks)
            def _():
                hidden(c, j)

            @pl.when(jnp.logical_and(c >= 1, j == FWD_AT))
            def _():
                forwards(c - 1)

            @pl.when(jnp.logical_and(c >= 2, j == FWD_AT))
            def _():
                passes(c - 2)

            @pl.when(jnp.logical_and(c >= 1, j == OWN_AT))
            def _():
                own(c - 1)

        @pl.when(c < chunks)
        def _():
            leaves(c)

    passes(chunks - 1)

    @pl.loop(chunks - 2, chunks)
    def _(c):
        for a in range(2):
            for k in range(3):
                rs_copy(c, k, a).wait_send()
                ag_copy(c, k, a).wait_send()

    @pl.loop(0, chunks)
    def _(c):
        for a in range(2):
            ag_copy(c, SECOND, a).wait_recv()
            ag_copy(c, PASS, a).wait_recv()


def solution(mesh):
    n = mesh.shape["tp"]

    def step(x, w_gate, w_up, w_down):
        rows, d_model = x.shape
        ff = w_gate.shape[1]
        chunks, half = rows // ROWS, d_model // n // 2
        assert n == 4 and rows % ROWS == 0 and ff % TILE == 0
        dma = pltpu.SemaphoreType.DMA
        flops = 6 * rows * d_model * ff
        return pl.pallas_call(
            functools.partial(kernel, n),
            out_shape=pltpu.VMEM((rows, d_model), BF16),
            in_specs=[pl.BlockSpec(memory_space=pl.ANY)] * 4,
            out_specs=pl.BlockSpec(memory_space=pltpu.VMEM),
            scratch_shapes=[
                pltpu.VMEM((2, ROWS, d_model), BF16),
                pltpu.VMEM((2, d_model, 2 * TILE), BF16),
                pltpu.VMEM((2, ff, half), BF16),
                pltpu.VMEM((2, ROWS, ff), BF16),
                pltpu.VMEM((2, 6, ROWS, half), BF16),
                pltpu.VMEM((chunks, 2, ROWS, half), BF16),
                dma((2,)), dma((2, 2)), dma((2,)),
                dma((2, 6)), dma((chunks, 6)), dma((2, 6)), dma((chunks, 6)),
            ],
            compiler_params=pltpu.CompilerParams(
                collective_id=0, has_side_effects=True, vmem_limit_bytes=45 * 1024 * 1024
            ),
            cost_estimate=pl.CostEstimate(
                flops=flops, bytes_accessed=chunks * 6 * d_model * ff, transcendentals=rows * ff
            ),
        )(x, w_gate, w_up, w_down)

    return jax.shard_map(
        step,
        mesh=mesh,
        in_specs=(P("dp", None), P(None, "tp"), P(None, "tp"), P("tp", None)),
        out_specs=P("dp", None),
        check_vma=False,
    )
```

```python
import functools

import jax
import jax.numpy as jnp
from jax import lax
from jax.experimental import pallas as pl
from jax.experimental.pallas import tpu as pltpu
from jax.sharding import PartitionSpec as P

MESH = pl.DeviceIdType.MESH
F32, BF16 = jnp.float32, jnp.bfloat16

ROWS = 256
TILE = 640
PARTS = 2
AHEAD = 3
D_SLOTS = 2
SUB = 2
FWD_AT, OWN_AT = 0, 2
FAR, NEAR, FWD = 0, 1, 2
FIRST, SECOND, PASS = 0, 1, 2


def kernel(
    n, x_hbm, wg_hbm, wu_hbm, wd_hbm, y_ref,
    xbuf, wbuf, dbuf, hbuf, sbuf, nbuf,
    x_sem, w_sem, d_sem, rs_send, rs_recv, ag_send, ag_recv,
):
    rows, d_model = x_hbm.shape
    ff = wg_hbm.shape[1]
    chunks, tiles = rows // ROWS, ff // TILE
    width = d_model // n
    half = width // 2
    depth = d_model // PARTS
    sub = ROWS // SUB
    me = lax.axis_index("tp")
    side = (lax.rem(me + n - 1, n), lax.rem(me + 1, n))
    far = lax.rem(me + 2, n)

    def rows_of(c, r=None):
        if r is None:
            return pl.ds(pl.multiple_of(c * ROWS, ROWS), ROWS)
        return pl.ds(pl.multiple_of(c * ROWS + r * sub, sub), sub)

    def cols_of(shard, h):
        return pl.ds(pl.multiple_of(shard * width + h * half, half), half)

    def x_copy(c):
        slot = lax.rem(c, 2)
        return pltpu.make_async_copy(x_hbm.at[rows_of(c), :], xbuf.at[slot], x_sem.at[slot])

    def w_copies(t):
        slot = lax.rem(t, AHEAD + 1)
        deep = pl.ds(pl.multiple_of(lax.rem(t, PARTS) * depth, depth), depth)
        cols = pl.ds(pl.multiple_of(lax.rem(t // PARTS, tiles) * TILE, TILE), TILE)
        return (
            pltpu.make_async_copy(wg_hbm.at[deep, cols], wbuf.at[slot, :, pl.ds(0, TILE)], w_sem.at[slot, 0]),
            pltpu.make_async_copy(wu_hbm.at[deep, cols], wbuf.at[slot, :, pl.ds(TILE, TILE)], w_sem.at[slot, 1]),
        )

    pieces = (
        (far, 0), (far, 1), (side[0], 1), (side[1], 0),
        (side[0], 0), (side[1], 1), (me, 0), (me, 1),
    )

    def d_copy(q):
        slot = q % D_SLOTS
        return pltpu.make_async_copy(wd_hbm.at[:, cols_of(*pieces[q])], dbuf.at[slot], d_sem.at[slot])

    def place(c, shard, h):
        return y_ref.at[rows_of(c), cols_of(shard, h)]

    def send(src, dst, send_sem, recv_sem, a):
        return pltpu.make_async_remote_copy(
            src_ref=src, dst_ref=dst, send_sem=send_sem, recv_sem=recv_sem,
            device_id={"tp": side[a]}, device_id_type=MESH,
        )

    def rs_copy(c, k, a, r=0):
        slot, i = lax.rem(c, 2), 2 * k + a
        src = sbuf.at[slot, i]
        if k == FAR:
            dst = place(c, far, a)
        elif k == NEAR:
            dst = nbuf.at[slot, a]
        else:
            src = sbuf.at[slot, i, pl.ds(r * sub, sub)]
            dst = y_ref.at[rows_of(c, r), cols_of(side[a], a)]
            i += 2 * r
        return send(src, dst, rs_send.at[slot, i], rs_recv.at[c, i], a)

    def ag_copy(c, k, a, r=0):
        if k == PASS:
            where = place(c, side[1 - a], a)
        elif k == SECOND:
            where = place(c, me, 1 - a)
        else:
            where = y_ref.at[rows_of(c, r), cols_of(me, a)]
        i = a + 2 * (r if k == FIRST else SUB - 1 + k)
        return send(where, where, ag_send.at[lax.rem(c, 2), i], ag_recv.at[c, i], a)

    def term(c, q, rows=slice(None)):
        return jnp.dot(hbuf[lax.rem(c, 2), rows], dbuf[q % D_SLOTS], preferred_element_type=F32)

    def refill(c, q):
        if q + D_SLOTS < len(pieces):
            d_copy(q + D_SLOTS).start()
        else:
            @pl.when(c + 1 < chunks)
            def _():
                d_copy(q + D_SLOTS - len(pieces)).start()

    def hidden(c, j):
        @pl.when(j == 0)
        def _():
            @pl.when(c + 1 < chunks)
            def _():
                x_copy(c + 1).start()
            x_copy(c).wait()

        both = None
        for p in range(PARTS):
            t = (c * tiles + j) * PARTS + p

            @pl.when(t + AHEAD < chunks * tiles * PARTS)
            def _():
                for copy in w_copies(t + AHEAD):
                    copy.start()

            for copy in w_copies(t):
                copy.wait()
            part = jnp.dot(
                xbuf[lax.rem(c, 2), :, p * depth : (p + 1) * depth],
                wbuf[lax.rem(t, AHEAD + 1)],
                preferred_element_type=F32,
            )
            both = part if p == 0 else both + part
        gate, up = both[:, :TILE], both[:, TILE:]
        cols = pl.ds(pl.multiple_of(j * TILE, TILE), TILE)
        hbuf[lax.rem(c, 2), :, cols] = (jax.nn.silu(gate) * up).astype(BF16)

    def free(c, *copies):
        @pl.when(c >= 2)
        def _():
            for copy, *which in copies:
                copy(c - 2, *which).wait_send()

    def leaves(c):
        for q in range(4):
            k, a = q // 2, q % 2
            free(c, (rs_copy, k, a))
            d_copy(q).wait()
            sbuf[lax.rem(c, 2), 2 * k + a] = term(c, q).astype(BF16)
            rs_copy(c, k, a).start()
            refill(c, q)

    def forwards(c):
        for r in range(SUB):
            part = slice(r * sub, (r + 1) * sub)
            for a in range(2):
                free(c, (rs_copy, FWD, a, r))
                if r == 0:
                    d_copy(4 + a).wait()
                    rs_copy(c, FAR, a).wait_recv()
                arrived = y_ref[rows_of(c, r), cols_of(side[a], a)].astype(F32)
                total = term(c, 4 + a, part) + arrived
                sbuf[lax.rem(c, 2), 2 * FWD + a, part] = total.astype(BF16)
                rs_copy(c, FWD, a, r).start()
                if r == SUB - 1:
                    refill(c, 4 + a)

    def own(c):
        for r in range(SUB):
            part = slice(r * sub, (r + 1) * sub)
            for h in range(2):
                free(c, (ag_copy, FIRST, h, r))
                if r == 0:
                    d_copy(6 + h).wait()
                    rs_copy(c, NEAR, 1 - h).wait_recv()
                rs_copy(c, FWD, h, r).wait_recv()
                at = (rows_of(c, r), cols_of(me, h))
                direct = nbuf[lax.rem(c, 2), 1 - h, part].astype(F32)
                y_ref[at] = (term(c, 6 + h, part) + direct + y_ref[at].astype(F32)).astype(BF16)
                ag_copy(c, FIRST, h, r).start()
                if r == SUB - 1:
                    refill(c, 6 + h)
        for a in range(2):
            free(c, (ag_copy, SECOND, a))
            ag_copy(c, SECOND, a).start()

    def passes(c):
        for a in range(2):
            free(c, (ag_copy, PASS, a))
            for r in range(SUB):
                ag_copy(c, FIRST, a, r).wait_recv()
            ag_copy(c, PASS, a).start()

    x_copy(0).start()
    for t in range(AHEAD):
        for copy in w_copies(t):
            copy.start()
    for q in range(D_SLOTS):
        d_copy(q).start()

    barrier = pltpu.get_barrier_semaphore()
    for a in range(2):
        pl.semaphore_signal(barrier, inc=1, device_id={"tp": side[a]}, device_id_type=MESH)
    pl.semaphore_wait(barrier, 2)

    @pl.loop(0, chunks + 1)
    def _(c):
        @pl.loop(0, tiles)
        def _(j):
            @pl.when(c < chunks)
            def _():
                hidden(c, j)

            @pl.when(jnp.logical_and(c >= 1, j == FWD_AT))
            def _():
                forwards(c - 1)

            @pl.when(jnp.logical_and(c >= 2, j == FWD_AT))
            def _():
                passes(c - 2)

            @pl.when(jnp.logical_and(c >= 1, j == OWN_AT))
            def _():
                own(c - 1)

        @pl.when(c < chunks)
        def _():
            leaves(c)

    passes(chunks - 1)

    @pl.loop(chunks - 2, chunks)
    def _(c):
        for a in range(2):
            for k in (FAR, NEAR):
                rs_copy(c, k, a).wait_send()
            for k in (SECOND, PASS):
                ag_copy(c, k, a).wait_send()
            for r in range(SUB):
                rs_copy(c, FWD, a, r).wait_send()
                ag_copy(c, FIRST, a, r).wait_send()

    @pl.loop(0, chunks)
    def _(c):
        for a in range(2):
            ag_copy(c, SECOND, a).wait_recv()
            ag_copy(c, PASS, a).wait_recv()


def solution(mesh):
    n = mesh.shape["tp"]

    def step(x, w_gate, w_up, w_down):
        rows, d_model = x.shape
        ff = w_gate.shape[1]
        chunks, half = rows // ROWS, d_model // n // 2
        assert n == 4 and rows % ROWS == 0 and ff % TILE == 0
        dma, kinds = pltpu.SemaphoreType.DMA, 4 + 2 * SUB
        flops = 6 * rows * d_model * ff
        return pl.pallas_call(
            functools.partial(kernel, n),
            out_shape=pltpu.VMEM((rows, d_model), BF16),
            in_specs=[pl.BlockSpec(memory_space=pl.ANY)] * 4,
            out_specs=pl.BlockSpec(memory_space=pltpu.VMEM),
            scratch_shapes=[
                pltpu.VMEM((2, ROWS, d_model), BF16),
                pltpu.VMEM((AHEAD + 1, d_model // PARTS, 2 * TILE), BF16),
                pltpu.VMEM((D_SLOTS, ff, half), BF16),
                pltpu.VMEM((2, ROWS, ff), BF16),
                pltpu.VMEM((2, 6, ROWS, half), BF16),
                pltpu.VMEM((2, 2, ROWS, half), BF16),
                dma((2,)), dma((AHEAD + 1, 2)), dma((D_SLOTS,)),
                dma((2, kinds)), dma((chunks, kinds)), dma((2, kinds)), dma((chunks, kinds)),
            ],
            compiler_params=pltpu.CompilerParams(
                collective_id=0, has_side_effects=True, vmem_limit_bytes=45 * 1024 * 1024
            ),
            cost_estimate=pl.CostEstimate(
                flops=flops, bytes_accessed=chunks * 6 * d_model * ff, transcendentals=rows * ff
            ),
        )(x, w_gate, w_up, w_down)

    return jax.shard_map(
        step,
        mesh=mesh,
        in_specs=(P("dp", None), P(None, "tp"), P(None, "tp"), P("tp", None)),
        out_specs=P("dp", None),
        check_vma=False,
    )
```
